256 devices in a mesh: sweep: 2 (over y), row: 16 (over z), col: 4 (over x), dp: 2 (over core).
Axes of the slice: x: 4, y: 2, z: 16, core: 2. Of those that a mesh axis runs over, the one named last changes fastest.
The devices are a block of a 4x16x16 slice.
Arguments:
- token_ids: int32 [4096], P(('sweep', 'dp')), parts along dimension 0, may hold values from 0 to 15999
- sweep_index: int32 [4], P('sweep'), parts along dimension 0, may hold values from 0 to 7
- table: bfloat16 [16000, 4096], P('row', 'col'), may hold values from -6 to 6
- cotangent: bfloat16 [4096, 4096], P(('sweep', 'dp', 'row'), 'col'), parts along dimension 0, may hold values from -0.13183594 to 0.13183594
- gate_weight: bfloat16 [4096, 11008], P('col', 'row'), may hold values from -0.09375 to 0.09375
- up_weight: bfloat16 [4096, 11008], P('col', 'row'), may hold values from -0.09375 to 0.09375
- down_weight: bfloat16 [11008, 4096], P('row', 'col'), may hold values from -0.0546875 to 0.0546875
Outputs:
- grad_gate: float32 [8192, 11008], P(('sweep', 'col'), ('row', 'dp')), parts along dimension 0
- grad_up: float32 [8192, 11008], P(('sweep', 'col'), ('row', 'dp')), parts along dimension 0
- grad_down: float32 [22016, 4096], P(('sweep', 'row'), ('col', 'dp')), parts along dimension 0
The draws below stay inside these ranges and needn't reach their ends.
There are 2 independent parts, one for each index of `sweep`. The reference program is written for one: setup_inputs(seed, part) draws one part's arguments, and reference() takes and returns one part's arrays. A program takes and returns all parts, laid end to end along the dimension named above; an argument that names none is the same for every part. Nothing has to cross between parts.
All inputs are finite; a program needn't handle non-finite values.
Results may differ from the reference program's by a relative error of at most 0.0062.
Values may be sent and summed in bfloat16 or wider, within the bound.
No kernel may reach another device: no remote copies, remote signals or barrier semaphores. Data moves between devices by JAX's collectives and lax.ppermute only.
A program may use at most 128 MiB of HBM per device.

```python
import math
import jax
import jax.numpy as jnp
import numpy as np

D = 4096
FF = 11008
VOCAB = 16000
TOKENS = 2048


def touch_ends(entries, own_key, smallest, top_value):
    dims = entries.shape
    place = [jax.random.randint(jax.random.fold_in(own_key, axis), (), 0, dims[axis]) for axis in range(len(dims))]
    entries = entries.at[tuple(place)].set(smallest)
    longest = dims.index(max(dims))
    place[longest] = (place[longest] + 1) % dims[longest]
    return entries.at[tuple(place)].set(top_value)


def levels(stream_key, extent, shards, smallest, high):
    loudness, own = 1.0, jax.random.fold_in(stream_key, 6)
    for position, blocks in shards:
        draws = jnp.exp(jax.random.uniform(jax.random.fold_in(own, position), (blocks,), jnp.float32, smallest / len(shards), high / len(shards)))
        loudness = loudness * jnp.repeat(draws, extent[position] // blocks).reshape([-1 if axis == position else 1 for axis in range(len(extent))])
    return loudness


def rank_bounds(amount, lean):
    weights = [(1 << 20) // math.isqrt(grade ** lean) + 1 for grade in range(1, amount + 1)]
    width = 1 + sum(weights) // (1 << 30)
    return np.cumsum(np.array([max(1, weight // width) for weight in weights]))


def ranked_ids(own_key, dims, amount, slope):
    listing = rank_bounds(amount, slope)
    lot = jax.random.randint(jax.random.fold_in(own_key, 1), dims, 0, int(listing[amount - 1]))
    grade = jnp.searchsorted(jnp.asarray(listing, jnp.int32), lot, side="right")
    return jax.random.permutation(jax.random.fold_in(own_key, 2), amount)[grade].astype(jnp.int32)


def noise(rng, shape, width, reach, split=(), kind=jnp.bfloat16):
    entries = width * jax.random.normal(rng, shape, jnp.float32)
    if split:
        entries = entries * levels(rng, shape, split, -0.22, 0.18)
    return jnp.clip(entries, -reach, reach).astype(kind)


def setup_inputs(seed: int = 0, part: int = 0) -> dict:
    arg_keys = jax.random.split(jax.random.key(seed), 8)
    part_keys = jax.random.split(jax.random.fold_in(arg_keys[7], part), 8)
    token_ids = touch_ends(ranked_ids(part_keys[0], (TOKENS,), VOCAB, 2), jax.random.fold_in(part_keys[0], 3), 0, VOCAB - 1).astype(jnp.int32)
    sweep_index = jax.random.randint(part_keys[1], (2,), 0, 8).astype(jnp.int32)
    table = noise(arg_keys[2], (VOCAB, D), 1.0, 6.0, ((0, 16), (1, 4)))
    cotangent = noise(part_keys[3], (TOKENS, D), (TOKENS ** -0.5), 0.13183594, ((0, 32), (1, 4)))
    gate_weight = noise(arg_keys[4], (D, FF), D ** -0.5, 0.09375, ((0, 4), (1, 16)))
    up_weight = noise(arg_keys[5], (D, FF), D ** -0.5, 0.09375, ((0, 4), (1, 16)))
    down_weight = noise(arg_keys[6], (FF, D), FF ** -0.5, 0.0546875, ((0, 16), (1, 4)))
    return {"token_ids": token_ids, "sweep_index": sweep_index, "table": table, "cotangent": cotangent, "gate_weight": gate_weight, "up_weight": up_weight, "down_weight": down_weight}


def reference(token_ids, sweep_index, table, cotangent, gate_weight, up_weight, down_weight):
    k_input = sweep_index[0].astype(jnp.float32)
    k_output = sweep_index[1].astype(jnp.float32)
    in_mult = jnp.exp2(k_input / 2.0 - 1.5)
    out_mult = jnp.exp2(1.0 - k_output / 2.0)
    embedded = jnp.take(table, token_ids, axis=0)
    scaled = (in_mult * embedded.astype(jnp.float32)).astype(jnp.bfloat16)
    gate = jnp.dot(scaled, gate_weight, preferred_element_type=jnp.float32)
    up = jnp.dot(scaled, up_weight, preferred_element_type=jnp.float32)
    back = out_mult * jnp.dot(cotangent, down_weight.T, preferred_element_type=jnp.float32)
    sig = jax.nn.sigmoid(gate)
    silu = gate * sig
    hidden = (silu * up).astype(jnp.bfloat16)
    d_gate = (back * up * sig * (1.0 + gate * (1.0 - sig))).astype(jnp.bfloat16)
    d_up = (back * silu).astype(jnp.bfloat16)
    grad_down = out_mult * jnp.dot(hidden.T, cotangent, preferred_element_type=jnp.float32)
    grad_gate = jnp.dot(scaled.T, d_gate, preferred_element_type=jnp.float32)
    grad_up = jnp.dot(scaled.T, d_up, preferred_element_type=jnp.float32)
    return grad_gate, grad_up, grad_down
```

```python
import jax
import jax.numpy as jnp
from jax import lax
from jax.experimental import pallas as pl
from jax.experimental.pallas import tpu as pltpu
from jax.sharding import PartitionSpec as P


F32 = jnp.float32
BF16 = jnp.bfloat16
GROUPS = 2
KERNEL_VMEM = 16 << 20


def shifted(x, axis, by):
    n = lax.axis_size(axis)
    return lax.ppermute(x, axis, [(i, (i + by) % n) for i in range(n)])


def on_chip(kernel, shapes, *operands):
    spec = pl.BlockSpec(memory_space=pltpu.VMEM)
    return pl.pallas_call(
        kernel,
        out_shape=[jax.ShapeDtypeStruct(s, BF16) for s in shapes],
        in_specs=[spec] * len(operands),
        out_specs=[spec] * len(shapes),
        compiler_params=pltpu.CompilerParams(vmem_limit_bytes=KERNEL_VMEM),
    )(*operands)


def far_kernel(mixed, back, top, bottom):
    n, h = back.shape[0], back.shape[0] // 2
    w = top.shape[1]
    lanes = slice(2 * w, 3 * w)
    top[:n] = mixed[:n, lanes].astype(BF16)
    top[n:] = back[:h, lanes].astype(BF16)
    bottom[:n] = mixed[n:, lanes].astype(BF16)
    bottom[n:] = back[h:, lanes].astype(BF16)


def near_kernel(mixed, back, from_left, from_right, right, left):
    n, h = back.shape[0], back.shape[0] // 2
    w = right.shape[1]
    for out, k, upper, lower in ((right, 1, from_left, None), (left, 3, None, from_right)):
        lanes = slice(k * w, (k + 1) * w)
        more = lambda ref, rows: 0.0 if ref is None else ref[rows].astype(F32)
        out[:n] = (mixed[:n, lanes] + more(upper, slice(0, n))).astype(BF16)
        out[n : 2 * n] = (mixed[n:, lanes] + more(lower, slice(0, n))).astype(BF16)
        out[2 * n : 2 * n + h] = (back[:h, lanes] + more(upper, slice(n, n + h))).astype(BF16)
        out[2 * n + h :] = (back[h:, lanes] + more(lower, slice(n, n + h))).astype(BF16)


def act_kernel(out_mult, mixed, back, a, b, out):
    n = back.shape[0]
    w = out.shape[1]
    gate = mixed[:n, :w] + (a[:n].astype(F32) + b[:n].astype(F32))
    up = mixed[n:, :w] + (a[n : 2 * n].astype(F32) + b[n : 2 * n].astype(F32))
    grad = out_mult[0, 0] * (back[:, :w] + (a[2 * n :].astype(F32) + b[2 * n :].astype(F32)))
    sig = jax.nn.sigmoid(gate)
    silu = gate * sig
    out[:n] = (silu * up).astype(BF16)
    out[n : 2 * n] = (grad * up * sig * (1.0 + gate * (1.0 - sig))).astype(BF16)
    out[2 * n :] = (grad * silu).astype(BF16)


def join_kernel(core, own, plus, minus, top, bottom, keep_h, keep_g, keep_u, send):
    n = keep_h.shape[0]
    h, w = n // 2, own.shape[1]
    split = top.shape[0]
    first = core[0, 0] == 0
    for k, ref in enumerate((own, plus, None, minus)):
        lanes = slice(k * w, (k + 1) * w)

        def rows(lo, hi):
            if ref is not None:
                return ref[lo:hi]
            if hi <= split:
                return top[lo:hi]
            if lo >= split:
                return bottom[lo - split : hi - split]
            return jnp.concatenate([top[lo:split], bottom[: hi - split]], 0)

        hidden = rows(0, n)
        keep_h[:, lanes] = hidden
        send[:n, lanes] = hidden
        for at, keep in ((n, keep_g), (2 * n, keep_u)):
            one, two = rows(at, at + h), rows(at + h, at + n)
            keep[:, lanes] = jnp.where(first, one, two)
            send[at - (at - n) // 2 : at - (at - n) // 2 + h, lanes] = jnp.where(first, two, one)


def dot(left, right, dims):
    return lax.dot_general(left, right, (dims, ((), ())), preferred_element_type=F32)


def local(token_ids, sweep_index, table, cotangent, gate_weight, up_weight, down_weight):
    k_input = sweep_index[0].astype(F32)
    k_output = sweep_index[1].astype(F32)
    in_mult = jnp.exp2(k_input / 2.0 - 1.5)
    out_mult = jnp.exp2(1.0 - k_output / 2.0)
    rows = lax.axis_size("row")
    cols = lax.axis_size("col")
    me = lax.axis_index("row")
    col = lax.axis_index("col")
    core = lax.axis_index("dp")
    vocab, feats = table.shape
    tokens = token_ids.shape[0]
    width = gate_weight.shape[1]
    per_row = tokens // rows
    cap = per_row
    group = tokens // GROUPS
    block = group // cols

    spin = [(col + o) % cols for o in range(cols)]

    def reorder(a):
        return a.reshape(GROUPS, cols, block)[:, jnp.stack(spin)].reshape(tokens)

    ids = reorder(token_ids)
    shard = ids // vocab
    low = shard * vocab
    place = jnp.arange(tokens, dtype=jnp.int32)
    seen = jnp.any((ids[:, None] == ids[None, :]) & (place[None, :] < place[:, None]), axis=1)
    fresh = jnp.where(seen, -1, ids)
    slot = jnp.sum(
        ((fresh[None, :] >= low[:, None]) & (fresh[None, :] < ids[:, None])).astype(jnp.int32), axis=1
    )
    fits = jnp.max(slot) < cap
    named = (shard == me)[None, :] & (slot[None, :] == jnp.arange(cap, dtype=jnp.int32)[:, None])
    wanted = jnp.max(jnp.where(named, (ids - low)[None, :], 0), axis=1)
    picked = table.at[wanted].get(mode="promise_in_bounds")
    picked = (in_mult * picked.astype(F32)).astype(BF16)
    both = lax.all_gather(jnp.concatenate([picked, cotangent], 0), "row", axis=0, tiled=True)
    both_rows = cap + per_row
    index = shard * cap + slot

    def from_slots():
        one_hot = (index[:, None] == jnp.arange(rows * cap, dtype=jnp.int32)[None, :]).astype(BF16)
        held = both.reshape(rows, both_rows, feats)[:, :cap].reshape(rows * cap, feats)
        return dot(held, one_hot, ((0,), (1,))).astype(BF16)

    def from_sum():
        local_row = token_ids - me * vocab
        inside = (local_row >= 0) & (local_row < vocab)
        own = table.at[jnp.clip(local_row, 0, vocab - 1)].get(mode="promise_in_bounds")
        own = jnp.where(inside[:, None], (in_mult * own.astype(F32)).astype(BF16), jnp.zeros((), BF16))

        def step(_, carry):
            moving = shifted(carry[0], "row", 1)
            return moving, carry[1] + moving

        total = lax.fori_loop(0, rows - 1, step, (own, own))[1]
        return total.at[reorder(place)].get(mode="promise_in_bounds").T

    x_t = lax.cond(fits, from_slots, from_sum)

    weights_t = jnp.concatenate([gate_weight.T, up_weight.T], 0)
    half = width // 2
    half_feats = feats // 2
    pick = lambda pair, other: jnp.where((core == 0) != other, pair[0], pair[1])
    scalar = lambda v: jnp.broadcast_to(v, (8, 128))
    out_mult_tile, core_tile = scalar(out_mult), scalar(core)
    work = [{} for _ in range(GROUPS)]
    cut = width + half
    spread = both.reshape(rows, both_rows, feats)
    row_blocks = block // per_row

    for g, w in enumerate(work):
        w["x"] = x_t[:, g * group : (g + 1) * group]
        w["c"] = jnp.concatenate(
            [
                lax.dynamic_slice(
                    spread, ((g * cols + o) * row_blocks, cap, 0), (row_blocks, per_row, feats)
                ).reshape(block, feats)
                for o in spin
            ],
            0,
        )
        w["back"] = dot(down_weight, w["c"], ((1,), (1,)))
        w["mixed"] = dot(weights_t, w["x"], ((1,), (0,)))
        top, bottom = on_chip(far_kernel, [(cut, block)] * 2, w["mixed"], w["back"])
        w["far"] = shifted(top, "col", 1), shifted(bottom, "col", -1)
    for w in work:
        right, left = on_chip(near_kernel, [(3 * width, block)] * 2, w["mixed"], w["back"], *w["far"])
        w["near"] = shifted(right, "col", 1), shifted(left, "col", -1)
    for w in work:
        w["own"], = on_chip(act_kernel, [(3 * width, block)], out_mult_tile, w["mixed"], w["back"], *w["near"])
        w["minus"], w["plus"] = shifted(w["own"], "col", 1), shifted(w["own"], "col", -1)
    for w in work:
        w["two"] = shifted(w["minus"][:cut], "col", 1), shifted(w["plus"][cut:], "col", -1)
    c_all = jnp.concatenate([w["c"] for w in work], 0)
    c_halves = [c_all[:, i * half_feats : (i + 1) * half_feats] for i in range(2)]
    own_c = pick(c_halves, False)
    peer_x = shifted(x_t, "dp", 1)
    peer_c = shifted(pick(c_halves, True), "dp", 1)
    grads = None
    for g, w in enumerate(work):
        keep_h, keep_g, keep_u, to_peer = on_chip(
            join_kernel,
            [(width, group), (half, group), (half, group), (2 * width, group)],
            core_tile, w["own"], w["plus"], w["minus"], *w["two"],
        )
        px = peer_x[:, g * group : (g + 1) * group]
        pc = peer_c[g * group : (g + 1) * group]
        c_own = own_c[g * group : (g + 1) * group]
        peer_h = shifted(to_peer, "dp", 1)
        new = [
            dot(w["x"], keep_g, ((1,), (1,))),
            dot(w["x"], keep_u, ((1,), (1,))),
            dot(keep_h, c_own, ((1,), (0,))),
        ]
        if grads is not None:
            new = [p + q for p, q in zip(grads, new)]
        grads = [
            new[0] + dot(px, peer_h[width : width + half], ((1,), (1,))),
            new[1] + dot(px, peer_h[width + half :], ((1,), (1,))),
            new[2] + dot(peer_h[:width], pc, ((1,), (0,))),
        ]
    return grads[0], grads[1], out_mult * grads[2]


def solution(mesh):
    return jax.shard_map(
        local,
        mesh=mesh,
        in_specs=(
            P(("sweep", "dp")),
            P("sweep"),
            P("row", "col"),
            P(("sweep", "dp", "row"), "col"),
            P("col", "row"),
            P("col", "row"),
            P("row", "col"),
        ),
        out_specs=(
            P(("sweep", "col"), ("row", "dp")),
            P(("sweep", "col"), ("row", "dp")),
            P(("sweep", "row"), ("col", "dp")),
        ),
        check_vma=False,
    )
```

```python
import jax
import jax.numpy as jnp
from jax import lax
from jax.experimental import pallas as pl
from jax.experimental.pallas import tpu as pltpu
from jax.sharding import PartitionSpec as P


F32 = jnp.float32
BF16 = jnp.bfloat16
GROUPS = 2
KERNEL_VMEM = 16 << 20


def shifted(x, axis, by):
    n = lax.axis_size(axis)
    return lax.ppermute(x, axis, [(i, (i + by) % n) for i in range(n)])


def turned(x, first):
    n = lax.axis_size("row")
    pairs = [(2 * i + core, 2 * ((i + (1 if core == first else -1)) % n) + core) for i in range(n) for core in range(2)]
    return lax.ppermute(x, ("row", "dp"), pairs)


def on_chip(kernel, shapes, *operands, scratch=(), scalars=0):
    spec = pl.BlockSpec(memory_space=pltpu.VMEM)
    return pl.pallas_call(
        kernel,
        out_shape=[jax.ShapeDtypeStruct(s, BF16) for s in shapes],
        in_specs=[pl.BlockSpec(memory_space=pltpu.SMEM)] * scalars + [spec] * (len(operands) - scalars),
        scratch_shapes=[pltpu.VMEM(s, BF16) for s in scratch],
        out_specs=[spec] * len(shapes),
        compiler_params=pltpu.CompilerParams(vmem_limit_bytes=KERNEL_VMEM),
    )(*operands)


def rest_kernel(*refs):
    *chunks, out = refs
    n = out.shape[0] // len(chunks)
    for k, ref in enumerate(chunks):
        out[k * n : (k + 1) * n] = ref[n:]


def lay_down(own, chunks, other, held):
    n = own.shape[0]
    held[:n] = own[...]
    for k, ref in enumerate(chunks):
        held[(k + 1) * n : (k + 2) * n] = ref[:n]
    held[(len(chunks) + 1) * n :] = other[...]


def rows_kernel(index, own, *refs):
    *chunks, other, out, held = refs
    lay_down(own, chunks, other, held)
    step = out.shape[0] // 4
    for b in range(4):
        rows = slice(b * step, (b + 1) * step)
        lane = lax.broadcasted_iota(jnp.int32, (step, held.shape[0]), 1)
        one_hot = (lane == index[rows]).astype(F32).astype(BF16)
        out[rows] = jnp.dot(one_hot, held[...], preferred_element_type=F32).astype(BF16)


def spin_kernel(col, own, *refs):
    *chunks, other, out, held = refs
    lay_down(own, chunks, other, held)
    cols = 4
    group = out.shape[0] // GROUPS
    size = group // cols
    for g in range(GROUPS):
        for o in range(cols):
            at = pl.multiple_of(g * group + lax.rem(col[0] + o, cols) * size, size)
            out[g * group + o * size : g * group + (o + 1) * size] = held[pl.ds(at, size)]


def grads_kernel(out_mult, x, px, c, pc, *refs):
    *hs, gate, up, down = refs
    kept, sent = hs[: 3 * GROUPS], hs[3 * GROUPS :]
    n, h = down.shape[0], gate.shape[1]
    size = x.shape[1] // GROUPS
    nt = (((1,), (1,)), ((), ()))
    rows = 256
    for r in range(0, gate.shape[0], rows):
        for at, out in ((0, gate), (1, up)):
            total = None
            for g in range(GROUPS):
                lanes = slice(g * size, (g + 1) * size)
                theirs = sent[g][n + at * h : n + (at + 1) * h]
                for left, right in ((x, kept[3 * g + 1 + at][...]), (px, theirs)):
                    part = lax.dot_general(left[r : r + rows, lanes], right, nt, preferred_element_type=F32)
                    total = part if total is None else total + part
            out[r : r + rows] = total
    for r in range(0, n, n // 2):
        total = None
        for g in range(GROUPS):
            lanes = slice(g * size, (g + 1) * size)
            for left, right in ((kept[3 * g], c), (sent[g], pc)):
                part = jnp.dot(left[r : r + n // 2], right[lanes], preferred_element_type=F32)
                total = part if total is None else total + part
        down[r : r + n // 2] = out_mult[0, 0] * total


def far_kernel(mixed, back, top, bottom):
    n, h = back.shape[0], back.shape[0] // 2
    w = top.shape[1]
    lanes = slice(2 * w, 3 * w)
    top[:n] = mixed[:n, lanes].astype(BF16)
    top[n:] = back[:h, lanes].astype(BF16)
    bottom[:n] = mixed[n:, lanes].astype(BF16)
    bottom[n:] = back[h:, lanes].astype(BF16)


def near_kernel(mixed, back, from_left, from_right, right, left):
    n, h = back.shape[0], back.shape[0] // 2
    w = right.shape[1]
    for out, k, upper, lower in ((right, 1, from_left, None), (left, 3, None, from_right)):
        lanes = slice(k * w, (k + 1) * w)
        more = lambda ref, rows: 0.0 if ref is None else ref[rows].astype(F32)
        out[:n] = (mixed[:n, lanes] + more(upper, slice(0, n))).astype(BF16)
        out[n : 2 * n] = (mixed[n:, lanes] + more(lower, slice(0, n))).astype(BF16)
        out[2 * n : 2 * n + h] = (back[:h, lanes] + more(upper, slice(n, n + h))).astype(BF16)
        out[2 * n + h :] = (back[h:, lanes] + more(lower, slice(n, n + h))).astype(BF16)


def act_kernel(out_mult, mixed, back, a, b, out):
    n = back.shape[0]
    w = out.shape[1]
    gate = mixed[:n, :w] + (a[:n].astype(F32) + b[:n].astype(F32))
    up = mixed[n:, :w] + (a[n : 2 * n].astype(F32) + b[n : 2 * n].astype(F32))
    grad = out_mult[0, 0] * (back[:, :w] + (a[2 * n :].astype(F32) + b[2 * n :].astype(F32)))
    sig = jax.nn.sigmoid(gate)
    silu = gate * sig
    out[:n] = (silu * up).astype(BF16)
    out[n : 2 * n] = (grad * up * sig * (1.0 + gate * (1.0 - sig))).astype(BF16)
    out[2 * n :] = (grad * silu).astype(BF16)


def join_kernel(core, own, plus, minus, top, bottom, keep_h, keep_g, keep_u, send):
    n = keep_h.shape[0]
    h, w = n // 2, own.shape[1]
    split = top.shape[0]
    first = core[0, 0] == 0
    for k, ref in enumerate((own, plus, None, minus)):
        lanes = slice(k * w, (k + 1) * w)

        def rows(lo, hi):
            if ref is not None:
                return ref[lo:hi]
            if hi <= split:
                return top[lo:hi]
            if lo >= split:
                return bottom[lo - split : hi - split]
            return jnp.concatenate([top[lo:split], bottom[: hi - split]], 0)

        hidden = rows(0, n)
        keep_h[:, lanes] = hidden
        send[:n, lanes] = hidden
        for at, keep in ((n, keep_g), (2 * n, keep_u)):
            one, two = rows(at, at + h), rows(at + h, at + n)
            keep[:, lanes] = jnp.where(first, one, two)
            send[at - (at - n) // 2 : at - (at - n) // 2 + h, lanes] = jnp.where(first, two, one)


def dot(left, right, dims):
    return lax.dot_general(left, right, (dims, ((), ())), preferred_element_type=F32)


def local(token_ids, sweep_index, table, cotangent, gate_weight, up_weight, down_weight):
    k_input = sweep_index[0].astype(F32)
    k_output = sweep_index[1].astype(F32)
    in_mult = jnp.exp2(k_input / 2.0 - 1.5)
    out_mult = jnp.exp2(1.0 - k_output / 2.0)
    rows = lax.axis_size("row")
    cols = lax.axis_size("col")
    me = lax.axis_index("row")
    col = lax.axis_index("col")
    core = lax.axis_index("dp")
    vocab, feats = table.shape
    tokens = token_ids.shape[0]
    width = gate_weight.shape[1]
    per_row = tokens // rows
    cap = per_row
    group = tokens // GROUPS
    block = group // cols

    reach = rows // 2
    way = 1 - 2 * core

    steps = jnp.arange(rows, dtype=jnp.int32)
    source = (me + way * jnp.where(steps <= reach, -steps, steps - reach)) % rows

    def reorder(a):
        a = a.reshape(rows, per_row)[source].reshape(GROUPS, cols, block)
        return a[:, (col + jnp.arange(cols, dtype=jnp.int32)) % cols].reshape(tokens)

    def rings(own, first, beside, at):
        chunk = jnp.concatenate([own, shifted(own, "dp", 1)], 0)
        got = []
        for k in range(1, reach + 1):
            if k == at:
                chunk, beside = lax.optimization_barrier((chunk, beside))
            chunk = turned(chunk if k < reach else chunk[: own.shape[0]], first)
            got.append(chunk)
        rest, = on_chip(rest_kernel, [((reach - 1) * own.shape[0], feats)], *got[:-1])
        return (own, *got, shifted(rest, "dp", 1)), beside

    c_parts, token_ids = rings(cotangent, 0, token_ids, 1)
    shard = token_ids // vocab
    low = shard * vocab
    place = jnp.arange(tokens, dtype=jnp.int32)
    seen = jnp.any((token_ids[:, None] == token_ids[None, :]) & (place[None, :] < place[:, None]), axis=1)
    fresh = jnp.where(seen, -1, token_ids)
    slot = jnp.sum(
        ((fresh[None, :] >= low[:, None]) & (fresh[None, :] < token_ids[:, None])).astype(jnp.int32), axis=1
    )
    fits = jnp.max(slot) < cap
    named = (shard == me)[None, :] & (slot[None, :] == jnp.arange(cap, dtype=jnp.int32)[:, None])
    wanted = jnp.max(jnp.where(named, (token_ids - low)[None, :], 0), axis=1)
    picked = table.at[wanted].get(mode="promise_in_bounds")
    picked = (in_mult * picked.astype(F32)).astype(BF16)

    weights_t = jnp.concatenate([gate_weight.T, up_weight.T], 0)
    x_parts, weights_t = rings(picked, 1, weights_t, reach // 2)
    tall = [(tokens, feats)]
    c_all, = on_chip(spin_kernel, tall, col.astype(jnp.int32).reshape(1), *c_parts, scratch=tall, scalars=1)
    away = (way * (shard - me)) % rows
    index = reorder(jnp.where(away <= reach, away, rows + reach - away) * cap + slot)
    x_fast, = on_chip(rows_kernel, tall, index.reshape(tokens, 1), *x_parts, scratch=tall)

    def from_sum(_):
        local_row = token_ids - me * vocab
        inside = (local_row >= 0) & (local_row < vocab)
        own = table.at[jnp.clip(local_row, 0, vocab - 1)].get(mode="promise_in_bounds")
        own = jnp.where(inside[:, None], (in_mult * own.astype(F32)).astype(BF16), jnp.zeros((), BF16))

        def step(_, carry):
            moving = shifted(carry[0], "row", 1)
            return moving, carry[1] + moving

        total = lax.fori_loop(0, rows - 1, step, (own, own))[1]
        return jnp.bool_(True), total.at[reorder(place)].get(mode="promise_in_bounds")

    x = lax.while_loop(lambda carry: ~carry[0], from_sum, (fits, x_fast))[1]

    half = width // 2
    half_feats = feats // 2
    pick = lambda pair, other: jnp.where((core == 0) != other, pair[0], pair[1])
    scalar = lambda v: jnp.broadcast_to(v, (8, 128))
    out_mult_tile, core_tile = scalar(out_mult), scalar(core)
    work = [{} for _ in range(GROUPS)]
    cut = width + half

    for g, w in enumerate(work):
        w["x"] = x[g * group : (g + 1) * group]
        w["c"] = c_all[g * group : (g + 1) * group]
        w["back"] = dot(down_weight, w["c"], ((1,), (1,)))
        w["mixed"] = dot(weights_t, w["x"], ((1,), (1,)))
        top, bottom = on_chip(far_kernel, [(cut, block)] * 2, w["mixed"], w["back"])
        w["far"] = shifted(top, "col", 1), shifted(bottom, "col", -1)
    for w in work:
        right, left = on_chip(near_kernel, [(3 * width, block)] * 2, w["mixed"], w["back"], *w["far"])
        w["near"] = shifted(right, "col", 1), shifted(left, "col", -1)
    for w in work:
        w["own"], = on_chip(act_kernel, [(3 * width, block)], out_mult_tile, w["mixed"], w["back"], *w["near"])
        w["minus"], w["plus"] = shifted(w["own"], "col", 1), shifted(w["own"], "col", -1)
    for w in work:
        w["two"] = shifted(w["minus"][:cut], "col", 1), shifted(w["plus"][cut:], "col", -1)
    c_halves = [c_all[:, i * half_feats : (i + 1) * half_feats] for i in range(2)]
    own_c = pick(c_halves, False)
    x_t = x.T
    peer_x = shifted(x_t, "dp", 1)
    peer_c = shifted(pick(c_halves, True), "dp", 1)
    kept, arrived = [], []
    for w in work:
        *keep, to_peer = on_chip(
            join_kernel,
            [(width, group), (half, group), (half, group), (2 * width, group)],
            core_tile, w["own"], w["plus"], w["minus"], *w["two"],
        )
        kept += keep
        arrived.append(shifted(to_peer, "dp", 1))
    operands = (out_mult_tile, x_t, peer_x, own_c, peer_c, *kept, *arrived)
    spec = pl.BlockSpec(memory_space=pltpu.VMEM)
    return tuple(
        pl.pallas_call(
            grads_kernel,
            out_shape=[
                jax.ShapeDtypeStruct(shape, F32) for shape in ((feats, half), (feats, half), (width, half_feats))
            ],
            in_specs=[spec] * len(operands),
            out_specs=[spec] * 3,
            compiler_params=pltpu.CompilerParams(vmem_limit_bytes=2 * KERNEL_VMEM),
        )(*operands)
    )


def solution(mesh):
    return jax.shard_map(
        local,
        mesh=mesh,
        in_specs=(
            P(("sweep", "dp")),
            P("sweep"),
            P("row", "col"),
            P(("sweep", "dp", "row"), "col"),
            P("col", "row"),
            P("col", "row"),
            P("row", "col"),
        ),
        out_specs=(
            P(("sweep", "col"), ("row", "dp")),
            P(("sweep", "col"), ("row", "dp")),
            P(("sweep", "row"), ("col", "dp")),
        ),
        check_vma=False,
    )
```

```python
import jax
import jax.numpy as jnp
from jax import lax
from jax.experimental import pallas as pl
from jax.experimental.pallas import tpu as pltpu
from jax.sharding import PartitionSpec as P


F32 = jnp.float32
BF16 = jnp.bfloat16
GROUPS = 2
KERNEL_VMEM = 16 << 20


def shifted(x, axis, by):
    n = lax.axis_size(axis)
    return lax.ppermute(x, axis, [(i, (i + by) % n) for i in range(n)])


def arrival_order(n):
    order = [0]
    for step in range(1, n // 2 + 1):
        order += [step] if 2 * step == n else [step, n - step]
    return order


def on_chip(kernel, shapes, *operands, scratch=(), scalars=0):
    spec = pl.BlockSpec(memory_space=pltpu.VMEM)
    return pl.pallas_call(
        kernel,
        out_shape=[jax.ShapeDtypeStruct(s, BF16) for s in shapes],
        in_specs=[pl.BlockSpec(memory_space=pltpu.SMEM)] * scalars + [spec] * (len(operands) - scalars),
        scratch_shapes=[pltpu.VMEM(s, BF16) for s in scratch],
        out_specs=[spec] * len(shapes),
        compiler_params=pltpu.CompilerParams(vmem_limit_bytes=KERNEL_VMEM),
    )(*operands)


def rows_kernel(source, fits, index, spare, *refs):
    chunks, outs = refs[: -2 - GROUPS], refs[-2 - GROUPS : -2]
    held, done = refs[-2:]
    n = held.shape[0] // len(chunks)
    for k, ref in enumerate(chunks):
        held[k * n : (k + 1) * n] = ref[:n]
    lanes = index.shape[1]
    per = source.shape[0] // GROUPS
    step = 4
    lane = lax.broadcasted_iota(jnp.int32, (n, lanes), 1).astype(F32)
    for g, out in enumerate(outs):
        for b in range(0, per, step):
            blocks = []
            for k in range(b, b + step):
                named = jnp.broadcast_to(index[pl.ds(source[g * per + k], 1)], (lanes, lanes)).T[:n]
                tiles = [(lane + t == named).astype(F32).astype(BF16) for t in range(0, held.shape[0], lanes)]
                blocks.append(jnp.concatenate(tiles, 1))
            rows = jnp.dot(jnp.concatenate(blocks, 0), held[...], preferred_element_type=F32)
            out[b * n : (b + step) * n] = rows.astype(BF16)

    @pl.when(fits[0] == 0)
    def _():
        for g, out in enumerate(outs):
            copy = pltpu.make_async_copy(spare.at[pl.ds(g * out.shape[0], out.shape[0])], out, done)
            copy.start()
            copy.wait()


def spin_kernel(place, *refs):
    *chunks, out, mine, theirs, held = refs
    n = held.shape[0] // len(chunks)
    for k, ref in enumerate(chunks):
        held[k * n : (k + 1) * n] = ref[ref.shape[0] - n :]
    cols = 4
    size = out.shape[0] // cols
    for o in range(cols):
        at = pl.multiple_of(lax.rem(place[0] + o, cols) * size, size)
        out[o * size : (o + 1) * size] = held[pl.ds(at, size)]
    half = mine.shape[1]
    first, second = out[:, :half], out[:, half:]
    mine[...] = jnp.where(place[1] == 0, first, second)
    theirs[...] = jnp.where(place[1] == 0, second, first)


def grads_kernel(out_mult, x, px, c, pc, *refs):
    *hs, gate, up, down = refs
    kept, sent = hs[: 3 * GROUPS], hs[3 * GROUPS :]
    n, h = down.shape[0], gate.shape[0]
    size = x.shape[0] // GROUPS
    for at, out in ((0, gate), (1, up)):
        total = None
        for g in range(GROUPS):
            lanes = slice(g * size, (g + 1) * size)
            theirs = sent[g][n + at * h : n + (at + 1) * h]
            for left, right in ((kept[3 * g + 1 + at][...], x), (theirs, px)):
                part = jnp.dot(left, right[lanes], preferred_element_type=F32)
                total = part if total is None else total + part
        out[...] = total
    for r in range(0, n, n // 2):
        total = None
        for g in range(GROUPS):
            lanes = slice(g * size, (g + 1) * size)
            for left, right in ((kept[3 * g], c), (sent[g], pc)):
                part = jnp.dot(left[r : r + n // 2], right[lanes], preferred_element_type=F32)
                total = part if total is None else total + part
        down[r : r + n // 2] = out_mult[0, 0] * total


def far_kernel(gate, up, back, top, bottom):
    n, h = back.shape[0], back.shape[0] // 2
    w = top.shape[1]
    lanes = slice(2 * w, 3 * w)
    top[:n] = gate[:, lanes].astype(BF16)
    top[n:] = back[:h, lanes].astype(BF16)
    bottom[:n] = up[:, lanes].astype(BF16)
    bottom[n:] = back[h:, lanes].astype(BF16)


def near_kernel(gate, up, back, from_left, from_right, right, left):
    n, h = back.shape[0], back.shape[0] // 2
    w = right.shape[1]
    for out, k, upper, lower in ((right, 1, from_left, None), (left, 3, None, from_right)):
        lanes = slice(k * w, (k + 1) * w)
        more = lambda ref, rows: 0.0 if ref is None else ref[rows].astype(F32)
        out[:n] = (gate[:, lanes] + more(upper, slice(0, n))).astype(BF16)
        out[n : 2 * n] = (up[:, lanes] + more(lower, slice(0, n))).astype(BF16)
        out[2 * n : 2 * n + h] = (back[:h, lanes] + more(upper, slice(n, n + h))).astype(BF16)
        out[2 * n + h :] = (back[h:, lanes] + more(lower, slice(n, n + h))).astype(BF16)


def act_kernel(out_mult, gates, ups, back, a, b, out):
    n = back.shape[0]
    w = out.shape[1]
    gate = gates[:, :w] + (a[:n].astype(F32) + b[:n].astype(F32))
    up = ups[:, :w] + (a[n : 2 * n].astype(F32) + b[n : 2 * n].astype(F32))
    grad = out_mult[0, 0] * (back[:, :w] + (a[2 * n :].astype(F32) + b[2 * n :].astype(F32)))
    sig = jax.nn.sigmoid(gate)
    silu = gate * sig
    out[:n] = (silu * up).astype(BF16)
    out[n : 2 * n] = (grad * up * sig * (1.0 + gate * (1.0 - sig))).astype(BF16)
    out[2 * n :] = (grad * silu).astype(BF16)


def join_kernel(core, own, plus, minus, top, bottom, keep_h, keep_g, keep_u, send):
    n = keep_h.shape[0]
    h, w = n // 2, own.shape[1]
    split = top.shape[0]
    first = core[0, 0] == 0
    for k, ref in enumerate((own, plus, None, minus)):
        lanes = slice(k * w, (k + 1) * w)

        def rows(lo, hi):
            if ref is not None:
                return ref[lo:hi]
            if hi <= split:
                return top[lo:hi]
            if lo >= split:
                return bottom[lo - split : hi - split]
            return jnp.concatenate([top[lo:split], bottom[: hi - split]], 0)

        hidden = rows(0, n)
        keep_h[:, lanes] = hidden
        send[:n, lanes] = hidden
        for at, keep in ((n, keep_g), (2 * n, keep_u)):
            one, two = rows(at, at + h), rows(at + h, at + n)
            keep[:, lanes] = jnp.where(first, one, two)
            send[at - (at - n) // 2 : at - (at - n) // 2 + h, lanes] = jnp.where(first, two, one)


def dot(left, right, dims):
    return lax.dot_general(left, right, (dims, ((), ())), preferred_element_type=F32)


def local(token_ids, sweep_index, table, cotangent, gate_weight, up_weight, down_weight):
    k_input = sweep_index[0].astype(F32)
    k_output = sweep_index[1].astype(F32)
    in_mult = jnp.exp2(k_input / 2.0 - 1.5)
    out_mult = jnp.exp2(1.0 - k_output / 2.0)
    rows = lax.axis_size("row")
    cols = lax.axis_size("col")
    me = lax.axis_index("row")
    col = lax.axis_index("col")
    core = lax.axis_index("dp")
    vocab, feats = table.shape
    tokens = token_ids.shape[0]
    width = gate_weight.shape[1]
    per_row = tokens // rows
    cap = per_row
    group = tokens // GROUPS
    half = width // 2
    half_feats = feats // 2
    block = group // cols

    order = arrival_order(rows)

    turn = jnp.arange(rows, dtype=jnp.int32).reshape(GROUPS, cols, -1)
    per_block = turn.shape[2]
    turn = turn - (turn // per_block) % cols * per_block
    turn = turn + (col + jnp.arange(cols, dtype=jnp.int32)[None, :, None]) % cols * per_block
    came = jnp.where(turn % 2 == 1, (turn + 1) // 2, (rows - turn // 2) % rows)
    source = ((me - came) % rows).reshape(rows)

    shard = token_ids // vocab
    low = shard * vocab
    spot = jnp.arange(tokens, dtype=jnp.int32)
    seen = jnp.any((token_ids[:, None] == token_ids[None, :]) & (spot[None, :] < spot[:, None]), axis=1)
    fresh = jnp.where(seen, -1, token_ids)
    slot = jnp.sum(
        ((fresh[None, :] >= low[:, None]) & (fresh[None, :] < token_ids[:, None])).astype(jnp.int32), axis=1
    )
    fits = jnp.max(slot) < cap
    named = (shard == me)[None, :] & (slot[None, :] == jnp.arange(cap, dtype=jnp.int32)[:, None])
    wanted = jnp.max(jnp.where(named, (token_ids - low)[None, :], 0), axis=1)
    picked = table.at[wanted].get(mode="promise_in_bounds")
    picked = (in_mult * picked.astype(F32)).astype(BF16)

    away = (me - shard) % rows
    at = jnp.where(2 * away <= rows, jnp.maximum(2 * away - 1, 0), 2 * (rows - away))
    index = (at * cap + slot).astype(F32).reshape(rows, per_row)
    index = jnp.concatenate([index, jnp.zeros_like(index)], 1)
    place = jnp.stack([col, core]).astype(jnp.int32)
    scalar = lambda v: jnp.broadcast_to(v, (8, 128))

    def from_sum(_):
        local_row = token_ids - me * vocab
        inside = (local_row >= 0) & (local_row < vocab)
        own = table.at[jnp.clip(local_row, 0, vocab - 1)].get(mode="promise_in_bounds")
        own = jnp.where(inside[:, None], (in_mult * own.astype(F32)).astype(BF16), jnp.zeros((), BF16))

        def step(_, carry):
            moving = shifted(carry[0], "row", 1)
            return moving, carry[1] + moving

        total = lax.fori_loop(0, rows - 1, step, (own, own))[1]
        listed = (source[:, None] * per_row + jnp.arange(per_row, dtype=jnp.int32)[None, :]).reshape(tokens)
        return jnp.bool_(True), total.at[listed].get(mode="promise_in_bounds")

    spare = lax.while_loop(lambda s: ~s[0], from_sum, (fits, jnp.zeros((tokens, feats), BF16)))[1]
    early = (picked, source, index, place, scalar(out_mult), scalar(core), fits.astype(jnp.int32).reshape(1), spare)
    picked, source, index, place, out_mult_tile, core_tile, flag, spare = lax.optimization_barrier(early)
    got = {0: jnp.concatenate([picked, cotangent], 0)}
    for k in range(1, rows // 2 + 1):
        ahead, behind = got[k - 1], got[(rows - k + 1) % rows]
        got[k] = shifted(ahead, "row", 1)
        if 2 * k < rows:
            got[rows - k] = shifted(behind, "row", -1)
    chunks = [got[k] for k in order]

    vmem, smem = (pl.BlockSpec(memory_space=m) for m in (pltpu.VMEM, pltpu.SMEM))
    xs = pl.pallas_call(
        rows_kernel,
        out_shape=[jax.ShapeDtypeStruct((group, feats), BF16)] * GROUPS,
        in_specs=[smem, smem, vmem, pl.BlockSpec(memory_space=pl.ANY)] + [vmem] * rows,
        out_specs=[vmem] * GROUPS,
        scratch_shapes=[pltpu.VMEM((rows * cap, feats), BF16), pltpu.SemaphoreType.DMA],
        compiler_params=pltpu.CompilerParams(vmem_limit_bytes=KERNEL_VMEM),
    )(source, flag, index, spare, *chunks)
    work = [{} for _ in range(GROUPS)]
    cut = width + half

    for g, w in enumerate(work):
        shape = [(group, feats)]
        per = len(chunks) // GROUPS
        mine = (group, half_feats)
        w["c"], w["mine"], w["theirs"] = on_chip(
            spin_kernel, shape + [mine] * 2, place, *chunks[g * per : (g + 1) * per], scratch=shape, scalars=1
        )
        w["x"] = xs[g]
        w["sums"] = (
            dot(gate_weight.T, w["x"], ((1,), (1,))),
            dot(up_weight.T, w["x"], ((1,), (1,))),
            dot(down_weight, w["c"], ((1,), (1,))),
        )
        top, bottom = on_chip(far_kernel, [(cut, block)] * 2, *w["sums"])
        w["far"] = shifted(top, "col", 1), shifted(bottom, "col", -1)
    for w in work:
        right, left = on_chip(near_kernel, [(3 * width, block)] * 2, *w["sums"], *w["far"])
        w["near"] = shifted(right, "col", 1), shifted(left, "col", -1)
    for w in work:
        w["own"], = on_chip(act_kernel, [(3 * width, block)], out_mult_tile, *w["sums"], *w["near"])
        w["minus"], w["plus"] = shifted(w["own"], "col", 1), shifted(w["own"], "col", -1)
    for w in work:
        w["two"] = shifted(w["minus"][:cut], "col", 1), shifted(w["plus"][cut:], "col", -1)
    x = jnp.concatenate([w["x"] for w in work], 0)
    peer_x = shifted(x, "dp", 1)
    peer_c = shifted(jnp.concatenate([w["theirs"] for w in work], 0), "dp", 1)
    kept, arrived = [], []
    for w in work:
        *keep, to_peer = on_chip(
            join_kernel,
            [(width, group), (half, group), (half, group), (2 * width, group)],
            core_tile, w["own"], w["plus"], w["minus"], *w["two"],
        )
        kept += keep
        arrived.append(shifted(to_peer, "dp", 1))
    operands = (out_mult_tile, x, peer_x, jnp.concatenate([w["mine"] for w in work], 0), peer_c, *kept, *arrived)
    spec = pl.BlockSpec(memory_space=pltpu.VMEM)
    gate_t, up_t, down = pl.pallas_call(
        grads_kernel,
        out_shape=[jax.ShapeDtypeStruct(shape, F32) for shape in ((half, feats), (half, feats), (width, half_feats))],
        in_specs=[spec] * len(operands),
        out_specs=[spec] * 3,
        compiler_params=pltpu.CompilerParams(vmem_limit_bytes=2 * KERNEL_VMEM),
    )(*operands)
    return gate_t.T, up_t.T, down


def solution(mesh):
    return jax.shard_map(
        local,
        mesh=mesh,
        in_specs=(
            P(("sweep", "dp")),
            P("sweep"),
            P("row", "col"),
            P(("sweep", "dp", "row"), "col"),
            P("col", "row"),
            P("col", "row"),
            P("row", "col"),
        ),
        out_specs=(
            P(("sweep", "col"), ("row", "dp")),
            P(("sweep", "col"), ("row", "dp")),
            P(("sweep", "row"), ("col", "dp")),
        ),
        check_vma=False,
    )
```

```python
import jax
import jax.numpy as jnp
from jax import lax
from jax.experimental import pallas as pl
from jax.experimental.pallas import tpu as pltpu
from jax.sharding import PartitionSpec as P


F32 = jnp.float32
BF16 = jnp.bfloat16
GROUPS = 2
KERNEL_VMEM = 16 << 20


def shifted(x, axis, by):
    n = lax.axis_size(axis)
    return lax.ppermute(x, axis, [(i, (i + by) % n) for i in range(n)])


def arrival_order(n):
    order = [0]
    for step in range(1, n // 2 + 1):
        order += [step] if 2 * step == n else [step, n - step]
    return order


def on_chip(kernel, shapes, *operands, scratch=(), scalars=0):
    spec = pl.BlockSpec(memory_space=pltpu.VMEM)
    return pl.pallas_call(
        kernel,
        out_shape=[jax.ShapeDtypeStruct(s, BF16) for s in shapes],
        in_specs=[pl.BlockSpec(memory_space=pltpu.SMEM)] * scalars + [spec] * (len(operands) - scalars),
        scratch_shapes=[pltpu.VMEM(s, BF16) for s in scratch],
        out_specs=[spec] * len(shapes),
        compiler_params=pltpu.CompilerParams(vmem_limit_bytes=KERNEL_VMEM),
    )(*operands)


def down_rows(row):
    return jnp.broadcast_to(row, (row.shape[1], row.shape[1])).T


def slots_kernel(own_low, ids, low, slot, wanted, top):
    count, n = ids.shape
    ahead = lax.broadcasted_iota(jnp.int32, (n, n), 0) < lax.broadcasted_iota(jnp.int32, (n, n), 1)
    row = lambda ref, b: ref[b : b + 1, :]
    down = [down_rows(row(ids, b)) for b in range(count)]
    fresh = []
    for t in range(count):
        hits = jnp.where((down[t] == row(ids, t)) & ahead, 1.0, 0.0)
        for b in range(t):
            hits = jnp.maximum(hits, jnp.where(down[b] == row(ids, t), 1.0, 0.0))
        fresh.append(down_rows(jnp.where(jnp.max(hits, axis=0, keepdims=True) > 0, -1.0, row(ids, t))))
    most = jnp.zeros((1, n), F32)
    found = jnp.zeros((n, n), F32)
    lane = lax.broadcasted_iota(jnp.int32, (n, n), 1).astype(F32)
    for t in range(count):
        less = jnp.zeros((n, n), F32)
        for b in range(count):
            less = less + jnp.where((fresh[b] >= row(low, t)) & (fresh[b] < row(ids, t)), 1.0, 0.0)
        rank = jnp.sum(less, axis=0, keepdims=True)
        slot[t : t + 1, :] = rank
        most = jnp.maximum(most, rank)
        mine = down_rows(jnp.where(row(low, t) == own_low[0], rank, -1.0))
        found = jnp.maximum(found, jnp.where(mine == lane, down[t] - own_low[0], 0.0))
    wanted[...] = jnp.max(found, axis=0, keepdims=True).astype(jnp.int32)
    top[...] = most


def pack_kernel(in_mult, picked, cotangent, out):
    n = picked.shape[0]
    out[:n] = (in_mult[0, 0] * picked[...].astype(F32)).astype(BF16)
    out[n:] = cotangent[...]


def rows_kernel(source, fits, index, spare, *refs):
    chunks, outs = refs[: -2 - GROUPS], refs[-2 - GROUPS : -2]
    held, done = refs[-2:]
    n = held.shape[0] // len(chunks)
    for k, ref in enumerate(chunks):
        held[k * n : (k + 1) * n] = ref[:n]
    lanes = index.shape[1]
    per = source.shape[0] // GROUPS
    step = 4
    lane = lax.broadcasted_iota(jnp.int32, (n, lanes), 1).astype(F32)
    for g, out in enumerate(outs):
        for b in range(0, per, step):
            blocks = []
            for k in range(b, b + step):
                row = source[g * per + k]
                named = down_rows(index[pl.ds(row // 2, 1)])
                named = jnp.where(row % 2 == 0, named[:n], named[n:])
                tiles = [(lane + t == named).astype(F32).astype(BF16) for t in range(0, held.shape[0], lanes)]
                blocks.append(jnp.concatenate(tiles, 1))
            rows = jnp.dot(jnp.concatenate(blocks, 0), held[...], preferred_element_type=F32)
            out[b * n : (b + step) * n] = rows.astype(BF16)

    @pl.when(fits[0] == 0)
    def _():
        for g, out in enumerate(outs):
            copy = pltpu.make_async_copy(spare.at[pl.ds(g * out.shape[0], out.shape[0])], out, done)
            copy.start()
            copy.wait()


def spin_kernel(place, *refs):
    *chunks, out, mine, theirs, held = refs
    n = held.shape[0] // len(chunks)
    for k, ref in enumerate(chunks):
        held[k * n : (k + 1) * n] = ref[ref.shape[0] - n :]
    cols = 4
    size = out.shape[0] // cols
    for o in range(cols):
        at = pl.multiple_of(lax.rem(place[0] + o, cols) * size, size)
        out[o * size : (o + 1) * size] = held[pl.ds(at, size)]
    half = mine.shape[1]
    first, second = out[:, :half], out[:, half:]
    mine[...] = jnp.where(place[1] == 0, first, second)
    theirs[...] = jnp.where(place[1] == 0, second, first)


def grads_kernel(out_mult, x, px, c, pc, *refs):
    *hs, gate, up, down = refs
    kept, sent = hs[: 3 * GROUPS], hs[3 * GROUPS :]
    n, h = down.shape[0], gate.shape[0]
    size = x.shape[0] // GROUPS
    for at, out in ((0, gate), (1, up)):
        total = None
        for g in range(GROUPS):
            lanes = slice(g * size, (g + 1) * size)
            theirs = sent[g][n + at * h : n + (at + 1) * h]
            for left, right in ((kept[3 * g + 1 + at][...], x), (theirs, px)):
                part = jnp.dot(left, right[lanes], preferred_element_type=F32)
                total = part if total is None else total + part
        out[...] = total
    for r in range(0, n, n // 2):
        total = None
        for g in range(GROUPS):
            lanes = slice(g * size, (g + 1) * size)
            for left, right in ((kept[3 * g], c), (sent[g], pc)):
                part = jnp.dot(left[r : r + n // 2], right[lanes], preferred_element_type=F32)
                total = part if total is None else total + part
        down[r : r + n // 2] = out_mult[0, 0] * total


def far_kernel(gate, up, back, top, bottom):
    n, h = back.shape[0], back.shape[0] // 2
    w = top.shape[1]
    lanes = slice(2 * w, 3 * w)
    top[:n] = gate[:, lanes].astype(BF16)
    top[n:] = back[:h, lanes].astype(BF16)
    bottom[:n] = up[:, lanes].astype(BF16)
    bottom[n:] = back[h:, lanes].astype(BF16)


def near_kernel(gate, up, back, from_left, from_right, right, left):
    n, h = back.shape[0], back.shape[0] // 2
    w = right.shape[1]
    for out, k, upper, lower in ((right, 1, from_left, None), (left, 3, None, from_right)):
        lanes = slice(k * w, (k + 1) * w)
        more = lambda ref, rows: 0.0 if ref is None else ref[rows].astype(F32)
        out[:n] = (gate[:, lanes] + more(upper, slice(0, n))).astype(BF16)
        out[n : 2 * n] = (up[:, lanes] + more(lower, slice(0, n))).astype(BF16)
        out[2 * n : 2 * n + h] = (back[:h, lanes] + more(upper, slice(n, n + h))).astype(BF16)
        out[2 * n + h :] = (back[h:, lanes] + more(lower, slice(n, n + h))).astype(BF16)


def act_kernel(out_mult, gates, ups, back, a, b, out):
    n = back.shape[0]
    w = out.shape[1]
    gate = gates[:, :w] + (a[:n].astype(F32) + b[:n].astype(F32))
    up = ups[:, :w] + (a[n : 2 * n].astype(F32) + b[n : 2 * n].astype(F32))
    grad = out_mult[0, 0] * (back[:, :w] + (a[2 * n :].astype(F32) + b[2 * n :].astype(F32)))
    sig = jax.nn.sigmoid(gate)
    silu = gate * sig
    out[:n] = (silu * up).astype(BF16)
    out[n : 2 * n] = (grad * up * sig * (1.0 + gate * (1.0 - sig))).astype(BF16)
    out[2 * n :] = (grad * silu).astype(BF16)


def join_kernel(core, own, plus, minus, top, bottom, keep_h, keep_g, keep_u, send):
    n = keep_h.shape[0]
    h, w = n // 2, own.shape[1]
    split = top.shape[0]
    first = core[0, 0] == 0
    for k, ref in enumerate((own, plus, None, minus)):
        lanes = slice(k * w, (k + 1) * w)

        def rows(lo, hi):
            if ref is not None:
                return ref[lo:hi]
            if hi <= split:
                return top[lo:hi]
            if lo >= split:
                return bottom[lo - split : hi - split]
            return jnp.concatenate([top[lo:split], bottom[: hi - split]], 0)

        hidden = rows(0, n)
        keep_h[:, lanes] = hidden
        send[:n, lanes] = hidden
        for at, keep in ((n, keep_g), (2 * n, keep_u)):
            one, two = rows(at, at + h), rows(at + h, at + n)
            keep[:, lanes] = jnp.where(first, one, two)
            send[at - (at - n) // 2 : at - (at - n) // 2 + h, lanes] = jnp.where(first, two, one)


def dot(left, right, dims):
    return lax.dot_general(left, right, (dims, ((), ())), preferred_element_type=F32)


def local(token_ids, sweep_index, table, cotangent, gate_weight, up_weight, down_weight):
    k_input = sweep_index[0].astype(F32)
    k_output = sweep_index[1].astype(F32)
    in_mult = jnp.exp2(k_input / 2.0 - 1.5)
    out_mult = jnp.exp2(1.0 - k_output / 2.0)
    rows = lax.axis_size("row")
    cols = lax.axis_size("col")
    me = lax.axis_index("row")
    col = lax.axis_index("col")
    core = lax.axis_index("dp")
    vocab, feats = table.shape
    tokens = token_ids.shape[0]
    width = gate_weight.shape[1]
    per_row = tokens // rows
    cap = per_row
    group = tokens // GROUPS
    half = width // 2
    half_feats = feats // 2
    block = group // cols

    order = arrival_order(rows)

    turn = jnp.arange(rows, dtype=jnp.int32).reshape(GROUPS, cols, -1)
    per_block = turn.shape[2]
    turn = turn - (turn // per_block) % cols * per_block
    turn = turn + (col + jnp.arange(cols, dtype=jnp.int32)[None, :, None]) % cols * per_block
    came = jnp.where(turn % 2 == 1, (turn + 1) // 2, (rows - turn // 2) % rows)
    source = ((me - came) % rows).reshape(rows)

    ids = token_ids.reshape(-1, 128)
    shard = ids // vocab
    low = (shard * vocab).astype(F32)
    vmem, smem = (pl.BlockSpec(memory_space=m) for m in (pltpu.VMEM, pltpu.SMEM))
    small = pltpu.CompilerParams(vmem_limit_bytes=KERNEL_VMEM)
    slot, wanted, top = pl.pallas_call(
        slots_kernel,
        out_shape=[
            jax.ShapeDtypeStruct(ids.shape, F32),
            jax.ShapeDtypeStruct((1, 128), jnp.int32),
            jax.ShapeDtypeStruct((1, 128), F32),
        ],
        in_specs=[smem, vmem, vmem],
        out_specs=[vmem] * 3,
        compiler_params=small,
    )((me * vocab).astype(F32).reshape(1), ids.astype(F32), low)
    fits = jnp.max(top) < cap
    picked = table.at[jnp.clip(wanted[0, :cap], 0, vocab - 1)].get(mode="promise_in_bounds")
    away = (me - shard) % rows
    at = jnp.where(2 * away <= rows, jnp.maximum(2 * away - 1, 0), 2 * (rows - away))
    index = (at * cap).astype(F32) + slot
    place = jnp.stack([col, core]).astype(jnp.int32)
    scalar = lambda v: jnp.broadcast_to(v, (8, 128))

    def from_sum(_):
        local_row = token_ids - me * vocab
        inside = (local_row >= 0) & (local_row < vocab)
        own = table.at[jnp.clip(local_row, 0, vocab - 1)].get(mode="promise_in_bounds")
        own = jnp.where(inside[:, None], (in_mult * own.astype(F32)).astype(BF16), jnp.zeros((), BF16))

        def step(_, carry):
            moving = shifted(carry[0], "row", 1)
            return moving, carry[1] + moving

        total = lax.fori_loop(0, rows - 1, step, (own, own))[1]
        listed = (source[:, None] * per_row + jnp.arange(per_row, dtype=jnp.int32)[None, :]).reshape(tokens)
        return jnp.bool_(True), total.at[listed].get(mode="promise_in_bounds")

    blank = pl.pallas_call(
        lambda ref: None,
        out_shape=jax.ShapeDtypeStruct((tokens, feats), BF16),
        out_specs=pl.BlockSpec(memory_space=pl.ANY),
        compiler_params=small,
    )()
    spare = lax.while_loop(lambda s: ~s[0], from_sum, (fits, blank))[1]
    scale = scalar(in_mult)
    first, = on_chip(pack_kernel, [(cap + per_row, feats)], scale, picked, cotangent)
    early = (first, source, index, place, scalar(out_mult), scalar(core), fits.astype(jnp.int32).reshape(1), spare)
    first, source, index, place, out_mult_tile, core_tile, flag, spare = lax.optimization_barrier(early)
    got = {0: first}
    for k in range(1, rows // 2 + 1):
        ahead, behind = got[k - 1], got[(rows - k + 1) % rows]
        got[k] = shifted(ahead, "row", 1)
        if 2 * k < rows:
            got[rows - k] = shifted(behind, "row", -1)
    chunks = [got[k] for k in order]

    xs = pl.pallas_call(
        rows_kernel,
        out_shape=[jax.ShapeDtypeStruct((group, feats), BF16)] * GROUPS,
        in_specs=[smem, smem, vmem, pl.BlockSpec(memory_space=pl.ANY)] + [vmem] * rows,
        out_specs=[vmem] * GROUPS,
        scratch_shapes=[pltpu.VMEM((rows * cap, feats), BF16), pltpu.SemaphoreType.DMA],
        compiler_params=pltpu.CompilerParams(vmem_limit_bytes=KERNEL_VMEM),
    )(source, flag, index, spare, *chunks)
    work = [{} for _ in range(GROUPS)]
    cut = width + half

    for g, w in enumerate(work):
        shape = [(group, feats)]
        per = len(chunks) // GROUPS
        mine = (group, half_feats)
        w["c"], w["mine"], w["theirs"] = on_chip(
            spin_kernel, shape + [mine] * 2, place, *chunks[g * per : (g + 1) * per], scratch=shape, scalars=1
        )
        w["x"] = xs[g]
        w["sums"] = (
            dot(gate_weight.T, w["x"], ((1,), (1,))),
            dot(up_weight.T, w["x"], ((1,), (1,))),
            dot(down_weight, w["c"], ((1,), (1,))),
        )
        top, bottom = on_chip(far_kernel, [(cut, block)] * 2, *w["sums"])
        w["far"] = shifted(top, "col", 1), shifted(bottom, "col", -1)
    for w in work:
        right, left = on_chip(near_kernel, [(3 * width, block)] * 2, *w["sums"], *w["far"])
        w["near"] = shifted(right, "col", 1), shifted(left, "col", -1)
    for w in work:
        w["own"], = on_chip(act_kernel, [(3 * width, block)], out_mult_tile, *w["sums"], *w["near"])
        w["minus"], w["plus"] = shifted(w["own"], "col", 1), shifted(w["own"], "col", -1)
    for w in work:
        w["two"] = shifted(w["minus"][:cut], "col", 1), shifted(w["plus"][cut:], "col", -1)
    x = jnp.concatenate([w["x"] for w in work], 0)
    peer_x = shifted(x, "dp", 1)
    peer_c = shifted(jnp.concatenate([w["theirs"] for w in work], 0), "dp", 1)
    kept, arrived = [], []
    for w in work:
        *keep, to_peer = on_chip(
            join_kernel,
            [(width, group), (half, group), (half, group), (2 * width, group)],
            core_tile, w["own"], w["plus"], w["minus"], *w["two"],
        )
        kept += keep
        arrived.append(shifted(to_peer, "dp", 1))
    operands = (out_mult_tile, x, peer_x, jnp.concatenate([w["mine"] for w in work], 0), peer_c, *kept, *arrived)
    spec = pl.BlockSpec(memory_space=pltpu.VMEM)
    gate_t, up_t, down = pl.pallas_call(
        grads_kernel,
        out_shape=[jax.ShapeDtypeStruct(shape, F32) for shape in ((half, feats), (half, feats), (width, half_feats))],
        in_specs=[spec] * len(operands),
        out_specs=[spec] * 3,
        compiler_params=pltpu.CompilerParams(vmem_limit_bytes=2 * KERNEL_VMEM),
    )(*operands)
    return gate_t.T, up_t.T, down


def solution(mesh):
    return jax.shard_map(
        local,
        mesh=mesh,
        in_specs=(
            P(("sweep", "dp")),
            P("sweep"),
            P("row", "col"),
            P(("sweep", "dp", "row"), "col"),
            P("col", "row"),
            P("col", "row"),
            P("row", "col"),
        ),
        out_specs=(
            P(("sweep", "col"), ("row", "dp")),
            P(("sweep", "col"), ("row", "dp")),
            P(("sweep", "row"), ("col", "dp")),
        ),
        check_vma=False,
    )
```

```python
import functools

import jax
import jax.numpy as jnp
from jax import lax
from jax.experimental import pallas as pl
from jax.experimental.pallas import tpu as pltpu
from jax.sharding import PartitionSpec as P


F32 = jnp.float32
BF16 = jnp.bfloat16
GROUPS = 2
KERNEL_VMEM = 16 << 20


def shifted(x, axis, by):
    n = lax.axis_size(axis)
    return lax.ppermute(x, axis, [(i, (i + by) % n) for i in range(n)])


def arrival_order(n):
    order = [0]
    for step in range(1, n // 2 + 1):
        order += [step] if 2 * step == n else [step, n - step]
    return order


def on_chip(kernel, shapes, *operands, scratch=(), scalars=0):
    spec = pl.BlockSpec(memory_space=pltpu.VMEM)
    return pl.pallas_call(
        kernel,
        out_shape=[jax.ShapeDtypeStruct(s, BF16) for s in shapes],
        in_specs=[pl.BlockSpec(memory_space=pltpu.SMEM)] * scalars + [spec] * (len(operands) - scalars),
        scratch_shapes=[pltpu.VMEM(s, BF16) for s in scratch],
        out_specs=[spec] * len(shapes),
        compiler_params=pltpu.CompilerParams(vmem_limit_bytes=KERNEL_VMEM),
    )(*operands)


def down_rows(row):
    return jnp.broadcast_to(row, (row.shape[1], row.shape[1])).T


def slots_kernel(own_low, ids, low, slot, wanted, top):
    count, n = ids.shape
    ahead = lax.broadcasted_iota(jnp.int32, (n, n), 0) < lax.broadcasted_iota(jnp.int32, (n, n), 1)
    row = lambda ref, b: ref[b : b + 1, :]
    down = [down_rows(row(ids, b)) for b in range(count)]
    fresh = []
    for t in range(count):
        hits = jnp.where((down[t] == row(ids, t)) & ahead, 1.0, 0.0)
        for b in range(t):
            hits = jnp.maximum(hits, jnp.where(down[b] == row(ids, t), 1.0, 0.0))
        fresh.append(down_rows(jnp.where(jnp.max(hits, axis=0, keepdims=True) > 0, -1.0, row(ids, t))))
    most = jnp.zeros((1, n), F32)
    found = jnp.zeros((n, n), F32)
    lane = lax.broadcasted_iota(jnp.int32, (n, n), 1).astype(F32)
    for t in range(count):
        less = jnp.zeros((n, n), F32)
        for b in range(count):
            less = less + jnp.where((fresh[b] >= row(low, t)) & (fresh[b] < row(ids, t)), 1.0, 0.0)
        rank = jnp.sum(less, axis=0, keepdims=True)
        slot[t : t + 1, :] = rank
        most = jnp.maximum(most, rank)
        mine = down_rows(jnp.where(row(low, t) == own_low[0], rank, -1.0))
        found = jnp.maximum(found, jnp.where(mine == lane, down[t] - own_low[0], 0.0))
    wanted[...] = jnp.max(found, axis=0, keepdims=True).astype(jnp.int32)
    top[...] = most


def pack_kernel(in_mult, picked, cotangent, out):
    n = picked.shape[0]
    out[:n] = (in_mult[0, 0] * picked[...].astype(F32)).astype(BF16)
    out[n:] = cotangent[...]


def rows_kernel(group, source, fits, index, spare, *refs):
    *chunks, out, held, done = refs
    n = held.shape[0] // len(chunks)
    for k, ref in enumerate(chunks):
        held[k * n : (k + 1) * n] = ref[:n]
    lanes = index.shape[1]
    per = source.shape[0] // GROUPS
    step = 4
    lane = lax.broadcasted_iota(jnp.int32, (n, lanes), 1).astype(F32)
    for b in range(0, per, step):
        blocks = []
        for k in range(b, b + step):
            row = source[group * per + k]
            named = down_rows(index[pl.ds(row // 2, 1)])
            named = jnp.where(row % 2 == 0, named[:n], named[n:])
            tiles = [(lane + t == named).astype(F32).astype(BF16) for t in range(0, held.shape[0], lanes)]
            blocks.append(jnp.concatenate(tiles, 1))
        rows = jnp.dot(jnp.concatenate(blocks, 0), held[...], preferred_element_type=F32)
        out[b * n : (b + step) * n] = rows.astype(BF16)

    @pl.when(fits[0] == 0)
    def _():
        copy = pltpu.make_async_copy(spare.at[pl.ds(group * out.shape[0], out.shape[0])], out, done)
        copy.start()
        copy.wait()


def spin_kernel(place, *refs):
    *chunks, out, mine, theirs, held = refs
    n = held.shape[0] // len(chunks)
    for k, ref in enumerate(chunks):
        held[k * n : (k + 1) * n] = ref[ref.shape[0] - n :]
    cols = 4
    size = out.shape[0] // cols
    for o in range(cols):
        at = pl.multiple_of(lax.rem(place[0] + o, cols) * size, size)
        out[o * size : (o + 1) * size] = held[pl.ds(at, size)]
    half = mine.shape[1]
    first, second = out[:, :half], out[:, half:]
    mine[...] = jnp.where(place[1] == 0, first, second)
    theirs[...] = jnp.where(place[1] == 0, second, first)


def grads_kernel(out_mult, x, px, c, pc, *refs):
    *hs, gate, up, down = refs
    kept, sent = hs[: 3 * GROUPS], hs[3 * GROUPS :]
    n, h = down.shape[0], gate.shape[0]
    size = x.shape[0] // GROUPS
    for at, out in ((0, gate), (1, up)):
        total = None
        for g in range(GROUPS):
            lanes = slice(g * size, (g + 1) * size)
            theirs = sent[g][n + at * h : n + (at + 1) * h]
            for left, right in ((kept[3 * g + 1 + at][...], x), (theirs, px)):
                part = jnp.dot(left, right[lanes], preferred_element_type=F32)
                total = part if total is None else total + part
        out[...] = total
    for r in range(0, n, n // 2):
        total = None
        for g in range(GROUPS):
            lanes = slice(g * size, (g + 1) * size)
            for left, right in ((kept[3 * g], c), (sent[g], pc)):
                part = jnp.dot(left[r : r + n // 2], right[lanes], preferred_element_type=F32)
                total = part if total is None else total + part
        down[r : r + n // 2] = out_mult[0, 0] * total


def far_kernel(gate, up, back, top, bottom):
    n, h = back.shape[0], back.shape[0] // 2
    w = top.shape[1]
    lanes = slice(2 * w, 3 * w)
    top[:n] = gate[:, lanes].astype(BF16)
    top[n:] = back[:h, lanes].astype(BF16)
    bottom[:n] = up[:, lanes].astype(BF16)
    bottom[n:] = back[h:, lanes].astype(BF16)


def near_kernel(gate, up, back, from_left, from_right, right, left):
    n, h = back.shape[0], back.shape[0] // 2
    w = right.shape[1]
    for out, k, upper, lower in ((right, 1, from_left, None), (left, 3, None, from_right)):
        lanes = slice(k * w, (k + 1) * w)
        more = lambda ref, rows: 0.0 if ref is None else ref[rows].astype(F32)
        out[:n] = (gate[:, lanes] + more(upper, slice(0, n))).astype(BF16)
        out[n : 2 * n] = (up[:, lanes] + more(lower, slice(0, n))).astype(BF16)
        out[2 * n : 2 * n + h] = (back[:h, lanes] + more(upper, slice(n, n + h))).astype(BF16)
        out[2 * n + h :] = (back[h:, lanes] + more(lower, slice(n, n + h))).astype(BF16)


def act_kernel(out_mult, gates, ups, back, a, b, out):
    n = back.shape[0]
    w = out.shape[1]
    gate = gates[:, :w] + (a[:n].astype(F32) + b[:n].astype(F32))
    up = ups[:, :w] + (a[n : 2 * n].astype(F32) + b[n : 2 * n].astype(F32))
    grad = out_mult[0, 0] * (back[:, :w] + (a[2 * n :].astype(F32) + b[2 * n :].astype(F32)))
    sig = jax.nn.sigmoid(gate)
    silu = gate * sig
    out[:n] = (silu * up).astype(BF16)
    out[n : 2 * n] = (grad * up * sig * (1.0 + gate * (1.0 - sig))).astype(BF16)
    out[2 * n :] = (grad * silu).astype(BF16)


def join_kernel(core, own, plus, minus, top, bottom, keep_h, keep_g, keep_u, send):
    n = keep_h.shape[0]
    h, w = n // 2, own.shape[1]
    split = top.shape[0]
    first = core[0, 0] == 0
    for k, ref in enumerate((own, plus, None, minus)):
        lanes = slice(k * w, (k + 1) * w)

        def rows(lo, hi):
            if ref is not None:
                return ref[lo:hi]
            if hi <= split:
                return top[lo:hi]
            if lo >= split:
                return bottom[lo - split : hi - split]
            return jnp.concatenate([top[lo:split], bottom[: hi - split]], 0)

        hidden = rows(0, n)
        keep_h[:, lanes] = hidden
        send[:n, lanes] = hidden
        for at, keep in ((n, keep_g), (2 * n, keep_u)):
            one, two = rows(at, at + h), rows(at + h, at + n)
            keep[:, lanes] = jnp.where(first, one, two)
            send[at - (at - n) // 2 : at - (at - n) // 2 + h, lanes] = jnp.where(first, two, one)


def dot(left, right, dims):
    return lax.dot_general(left, right, (dims, ((), ())), preferred_element_type=F32)


def local(token_ids, sweep_index, table, cotangent, gate_weight, up_weight, down_weight):
    k_input = sweep_index[0].astype(F32)
    k_output = sweep_index[1].astype(F32)
    in_mult = jnp.exp2(k_input / 2.0 - 1.5)
    out_mult = jnp.exp2(1.0 - k_output / 2.0)
    rows = lax.axis_size("row")
    cols = lax.axis_size("col")
    me = lax.axis_index("row")
    col = lax.axis_index("col")
    core = lax.axis_index("dp")
    vocab, feats = table.shape
    tokens = token_ids.shape[0]
    width = gate_weight.shape[1]
    per_row = tokens // rows
    cap = per_row
    group = tokens // GROUPS
    half = width // 2
    half_feats = feats // 2
    block = group // cols

    order = arrival_order(rows)

    turn = jnp.arange(rows, dtype=jnp.int32).reshape(GROUPS, cols, -1)
    per_block = turn.shape[2]
    turn = turn - (turn // per_block) % cols * per_block
    turn = turn + (col + jnp.arange(cols, dtype=jnp.int32)[None, :, None]) % cols * per_block
    came = jnp.where(turn % 2 == 1, (turn + 1) // 2, (rows - turn // 2) % rows)
    source = ((me - came) % rows).reshape(rows)

    ids = token_ids.reshape(-1, 128)
    shard = ids // vocab
    low = (shard * vocab).astype(F32)
    vmem, smem = (pl.BlockSpec(memory_space=m) for m in (pltpu.VMEM, pltpu.SMEM))
    small = pltpu.CompilerParams(vmem_limit_bytes=KERNEL_VMEM)
    slot, wanted, top = pl.pallas_call(
        slots_kernel,
        out_shape=[
            jax.ShapeDtypeStruct(ids.shape, F32),
            jax.ShapeDtypeStruct((1, 128), jnp.int32),
            jax.ShapeDtypeStruct((1, 128), F32),
        ],
        in_specs=[smem, vmem, vmem],
        out_specs=[vmem] * 3,
        compiler_params=small,
    )((me * vocab).astype(F32).reshape(1), ids.astype(F32), low)
    fits = jnp.max(top) < cap
    picked = table.at[jnp.clip(wanted[0, :cap], 0, vocab - 1)].get(mode="promise_in_bounds")
    away = (me - shard) % rows
    at = jnp.where(2 * away <= rows, jnp.maximum(2 * away - 1, 0), 2 * (rows - away))
    index = (at * cap).astype(F32) + slot
    place = jnp.stack([col, core]).astype(jnp.int32)
    scalar = lambda v: jnp.broadcast_to(v, (8, 128))

    def from_sum(_):
        local_row = token_ids - me * vocab
        inside = (local_row >= 0) & (local_row < vocab)
        own = table.at[jnp.clip(local_row, 0, vocab - 1)].get(mode="promise_in_bounds")
        own = jnp.where(inside[:, None], (in_mult * own.astype(F32)).astype(BF16), jnp.zeros((), BF16))

        def step(_, carry):
            moving = shifted(carry[0], "row", 1)
            return moving, carry[1] + moving

        total = lax.fori_loop(0, rows - 1, step, (own, own))[1]
        listed = (source[:, None] * per_row + jnp.arange(per_row, dtype=jnp.int32)[None, :]).reshape(tokens)
        return jnp.bool_(True), total.at[listed].get(mode="promise_in_bounds")

    blank = pl.pallas_call(
        lambda ref: None,
        out_shape=jax.ShapeDtypeStruct((tokens, feats), BF16),
        out_specs=pl.BlockSpec(memory_space=pl.ANY),
        compiler_params=small,
    )()
    spare = lax.while_loop(lambda s: ~s[0], from_sum, (fits, blank))[1]
    scale = scalar(in_mult)
    first, = on_chip(pack_kernel, [(cap + per_row, feats)], scale, picked, cotangent)
    early = (first, source, index, place, scalar(out_mult), scalar(core), fits.astype(jnp.int32).reshape(1), spare)
    first, source, index, place, out_mult_tile, core_tile, flag, spare = lax.optimization_barrier(early)
    got = {0: first}
    for k in range(1, rows // 2 + 1):
        ahead, behind = got[k - 1], got[(rows - k + 1) % rows]
        got[k] = shifted(ahead, "row", 1)
        if 2 * k < rows:
            got[rows - k] = shifted(behind, "row", -1)
    chunks = [got[k] for k in order]

    def table_rows(g, index):
        return pl.pallas_call(
            functools.partial(rows_kernel, g),
            out_shape=jax.ShapeDtypeStruct((group, feats), BF16),
            in_specs=[smem, smem, vmem, pl.BlockSpec(memory_space=pl.ANY)] + [vmem] * rows,
            out_specs=vmem,
            scratch_shapes=[pltpu.VMEM((rows * cap, feats), BF16), pltpu.SemaphoreType.DMA],
            compiler_params=small,
        )(source, flag, index, spare, *chunks)

    work = [{} for _ in range(GROUPS)]
    cut = width + half

    for g, w in enumerate(work):
        shape = [(group, feats)]
        per = len(chunks) // GROUPS
        mine = (group, half_feats)
        w["c"], w["mine"], w["theirs"] = on_chip(
            spin_kernel, shape + [mine] * 2, place, *chunks[g * per : (g + 1) * per], scratch=shape, scalars=1
        )
        w["x"] = table_rows(g, index)
        w["sums"] = (
            dot(gate_weight.T, w["x"], ((1,), (1,))),
            dot(up_weight.T, w["x"], ((1,), (1,))),
            dot(down_weight, w["c"], ((1,), (1,))),
        )
        top, bottom = on_chip(far_kernel, [(cut, block)] * 2, *w["sums"])
        index, top, bottom = lax.optimization_barrier((index, top, bottom))
        w["far"] = shifted(top, "col", 1), shifted(bottom, "col", -1)
    for w in work:
        right, left = on_chip(near_kernel, [(3 * width, block)] * 2, *w["sums"], *w["far"])
        w["near"] = shifted(right, "col", 1), shifted(left, "col", -1)
    for w in work:
        w["own"], = on_chip(act_kernel, [(3 * width, block)], out_mult_tile, *w["sums"], *w["near"])
        w["minus"], w["plus"] = shifted(w["own"], "col", 1), shifted(w["own"], "col", -1)
    for w in work:
        w["two"] = shifted(w["minus"][:cut], "col", 1), shifted(w["plus"][cut:], "col", -1)
    x = jnp.concatenate([w["x"] for w in work], 0)
    peer_x = shifted(x, "dp", 1)
    peer_c = shifted(jnp.concatenate([w["theirs"] for w in work], 0), "dp", 1)
    kept, arrived = [], []
    for w in work:
        *keep, to_peer = on_chip(
            join_kernel,
            [(width, group), (half, group), (half, group), (2 * width, group)],
            core_tile, w["own"], w["plus"], w["minus"], *w["two"],
        )
        kept += keep
        arrived.append(shifted(to_peer, "dp", 1))
    operands = (out_mult_tile, x, peer_x, jnp.concatenate([w["mine"] for w in work], 0), peer_c, *kept, *arrived)
    spec = pl.BlockSpec(memory_space=pltpu.VMEM)
    gate_t, up_t, down = pl.pallas_call(
        grads_kernel,
        out_shape=[jax.ShapeDtypeStruct(shape, F32) for shape in ((half, feats), (half, feats), (width, half_feats))],
        in_specs=[spec] * len(operands),
        out_specs=[spec] * 3,
        compiler_params=pltpu.CompilerParams(vmem_limit_bytes=2 * KERNEL_VMEM),
    )(*operands)
    return gate_t.T, up_t.T, down


def solution(mesh):
    return jax.shard_map(
        local,
        mesh=mesh,
        in_specs=(
            P(("sweep", "dp")),
            P("sweep"),
            P("row", "col"),
            P(("sweep", "dp", "row"), "col"),
            P("col", "row"),
            P("col", "row"),
            P("row", "col"),
        ),
        out_specs=(
            P(("sweep", "col"), ("row", "dp")),
            P(("sweep", "col"), ("row", "dp")),
            P(("sweep", "row"), ("col", "dp")),
        ),
        check_vma=False,
    )
```
